16 devices in a mesh: data: 16 (over z, y, x, core).
Axes of the slice: x: 2, y: 2, z: 2, core: 2. Of those that a mesh axis runs over, the one named last changes fastest.
Arguments:
- w_in: float32 [16, 512, 2048], replicated
- w_out: float32 [16, 2048, 512], replicated
- mom_in: float32 [16, 512, 2048], replicated
- mom_out: float32 [16, 2048, 512], replicated
- x_first: bfloat16 [8192, 512], P('data')
- y_first: bfloat16 [8192, 512], P('data')
- x_second: bfloat16 [8192, 512], P('data')
- y_second: bfloat16 [8192, 512], P('data')
Outputs:
- output 1: float32 [16, 512, 2048], replicated
- output 2: float32 [16, 2048, 512], replicated
- output 3: float32 [16, 512, 2048], replicated
- output 4: float32 [16, 2048, 512], replicated
- output 5: float32 [8192], P('data')
- output 6: float32 [8192, 512], P('data')
All inputs are finite; a program needn't handle non-finite values.
Results may differ from the reference program's by a relative error of at most 0.00755277.
Values are sent between devices in bfloat16 or wider.
A program may use at most 2.25 GiB of HBM per device.

```python
import jax
import jax.numpy as jnp
from jax import lax

MODEL_DIM = 512
HIDDEN_DIM = 2048
NUM_LAYERS = 16
TOK_DEV = 512
GROUP_SIZE = 16

LR_SCALE = 1.0
MOMENTUM = 0.9


def setup_inputs(seed: int = 0) -> dict:
    base_key = jax.random.key(seed)
    sub_keys = jax.random.split(base_key, 16)
    batch_rows = TOK_DEV * GROUP_SIZE
    shape_in = (NUM_LAYERS, MODEL_DIM, HIDDEN_DIM)
    shape_out = (NUM_LAYERS, HIDDEN_DIM, MODEL_DIM)
    w_in = jax.random.normal(sub_keys[0], shape_in, jnp.float32) * MODEL_DIM ** -0.5
    w_out = jax.random.normal(sub_keys[1], shape_out, jnp.float32) * (HIDDEN_DIM * NUM_LAYERS) ** -0.5
    mom_in = jax.random.normal(sub_keys[2], shape_in, jnp.float32) * (0.1 * NUM_LAYERS * MODEL_DIM ** -0.5)
    col_part = jax.random.normal(sub_keys[3], (NUM_LAYERS, 1, MODEL_DIM), jnp.float32)
    mom_out = (col_part + jax.random.normal(sub_keys[4], shape_out, jnp.float32)) / HIDDEN_DIM

    def draw_batch(key_list):
        x_mean = 0.7 * jax.random.normal(key_list[0], (1, MODEL_DIM), jnp.float32)
        x_vals = jax.random.normal(key_list[1], (batch_rows, MODEL_DIM), jnp.float32) + x_mean
        shared_off = jax.random.normal(key_list[2], (1, 1, MODEL_DIM), jnp.float32)
        dev_off = jax.random.normal(key_list[3], (GROUP_SIZE, 1, MODEL_DIM), jnp.float32)
        noise_part = 0.5 * jax.random.normal(key_list[4], (GROUP_SIZE, TOK_DEV, MODEL_DIM), jnp.float32)
        y_vals = (noise_part + shared_off + dev_off).reshape(batch_rows, MODEL_DIM)
        return x_vals.astype(jnp.bfloat16), y_vals.astype(jnp.bfloat16)

    x_first, y_first = draw_batch(sub_keys[5:10])
    x_second, y_second = draw_batch(sub_keys[10:15])
    return {"w_in": w_in, "w_out": w_out, "mom_in": mom_in, "mom_out": mom_out, "x_first": x_first, "y_first": y_first, "x_second": x_second, "y_second": y_second}


def forward_stack(w_in_bf, w_out_bf, h_start):
    def layer_step(h_cur, weights):
        w_in_l, w_out_l = weights
        h_bf = h_cur.astype(jnp.bfloat16)
        pre_act = jnp.dot(h_bf, w_in_l, preferred_element_type=jnp.float32)
        act_bf = jax.nn.gelu(pre_act).astype(jnp.bfloat16)
        h_next = h_cur + jnp.dot(act_bf, w_out_l, preferred_element_type=jnp.float32)
        return h_next, (h_bf, pre_act, act_bf)
    return lax.scan(layer_step, h_start, (w_in_bf, w_out_bf))


def device_grads(w_in_bf, w_out_bf, x_rows, y_rows):
    h_last, saved_acts = forward_stack(w_in_bf, w_out_bf, x_rows.astype(jnp.float32))
    inv_scale = 1.0 / (TOK_DEV * GROUP_SIZE * MODEL_DIM)
    err_last = (h_last - y_rows.astype(jnp.float32)) * inv_scale

    def back_step(err_row, layer_data):
        w_in_l, w_out_l, h_bf, pre_act, act_bf = layer_data
        err_bf = err_row.astype(jnp.bfloat16)
        grad_out = jnp.dot(act_bf.T, err_bf, preferred_element_type=jnp.float32)
        d_act = jnp.dot(err_bf, w_out_l.T, preferred_element_type=jnp.float32)
        gelu_back = jax.vjp(jax.nn.gelu, pre_act)[1]
        d_pre = gelu_back(d_act)[0].astype(jnp.bfloat16)
        grad_in = jnp.dot(h_bf.T, d_pre, preferred_element_type=jnp.float32)
        err_prev = err_row + jnp.dot(d_pre, w_in_l.T, preferred_element_type=jnp.float32)
        return err_prev, (grad_in.astype(jnp.bfloat16), grad_out.astype(jnp.bfloat16))

    err_first, grads = lax.scan(back_step, err_last, (w_in_bf, w_out_bf, saved_acts[0], saved_acts[1], saved_acts[2]), reverse=True)
    return grads


def reference(w_in, w_out, mom_in, mom_out, x_first, y_first, x_second, y_second):
    w_in_bf = w_in.astype(jnp.bfloat16)
    w_out_bf = w_out.astype(jnp.bfloat16)
    x_blocks = x_first.reshape(GROUP_SIZE, TOK_DEV, MODEL_DIM)
    y_blocks = y_first.reshape(GROUP_SIZE, TOK_DEV, MODEL_DIM)

    def add_device(grad_sums, block_pair):
        grad_in, grad_out = device_grads(w_in_bf, w_out_bf, block_pair[0], block_pair[1])
        return (grad_sums[0] + grad_in.astype(jnp.float32), grad_sums[1] + grad_out.astype(jnp.float32)), None

    zero_sums = (jnp.zeros(w_in.shape, jnp.float32), jnp.zeros(w_out.shape, jnp.float32))
    grad_sums, unused = lax.scan(add_device, zero_sums, (x_blocks, y_blocks))
    step_size = LR_SCALE / NUM_LAYERS
    mom_in_new = MOMENTUM * mom_in + grad_sums[0]
    mom_out_new = MOMENTUM * mom_out + grad_sums[1]
    w_in_new = w_in - step_size * mom_in_new
    w_out_new = w_out - step_size * mom_out_new
    new_in_bf = w_in_new.astype(jnp.bfloat16)
    new_out_bf = w_out_new.astype(jnp.bfloat16)

    def next_forward(x_rows):
        h_last, saved_acts = forward_stack(new_in_bf, new_out_bf, x_rows.astype(jnp.float32))
        return h_last

    h_blocks = lax.map(next_forward, x_second.reshape(GROUP_SIZE, TOK_DEV, MODEL_DIM))
    h_final = h_blocks.reshape(GROUP_SIZE * TOK_DEV, MODEL_DIM)
    row_diff = h_final - y_second.astype(jnp.float32)
    loss_rows = jnp.sum(row_diff * row_diff, axis=-1) / (2 * MODEL_DIM)
    return (w_in_new, w_out_new, mom_in_new, mom_out_new, loss_rows, h_final)
```

```python
import functools

import jax
import jax.numpy as jnp
from jax import lax
from jax.experimental import pallas as pl
from jax.experimental.pallas import tpu as pltpu
from jax.sharding import PartitionSpec as P

MESH = pl.DeviceIdType.MESH
BF = jnp.bfloat16
F32 = jnp.float32
LAYERS, DIM, HID, ROWS = 16, 512, 2048, 512
TILE = 512
PER = HID // TILE
UNITS = LAYERS * PER
STEP = 1.0 / LAYERS
MU = 0.9
C0 = 0.7978845608028654
C1 = C0 * 0.044715
BLOCK = (160, 160, 192)
START = (0, 160, 320)
HALF = (80, 80, 96)
HSTART = (0, 80, 160)
RING = 8
CHUNKS = ((0, 8), (8, 13), (13, 16))
VMEM_LIMIT = 60 * 2**20


def dot(a, b, ca=1, cb=0):
    return lax.dot_general(a, b, (((ca,), (cb,)), ((), ())), preferred_element_type=F32)


def gelu(z):
    t = jnp.tanh(z * (C0 + C1 * (z * z)))
    return z * (0.5 * t + 0.5)


def gelu_both(z):
    z2 = z * z
    t = jnp.tanh(z * (C0 + C1 * z2))
    cdf = 0.5 * t + 0.5
    return z * cdf, cdf + (0.5 * z) * ((1.0 - t * t) * (C0 + (3.0 * C1) * z2))


def axis_peer(me, order):
    stride = order * order + order + 2
    bit = lax.rem(lax.div(me, stride), 2)
    return bit, me + (1 - 2 * bit) * stride


def fwd_kernel(tiles, x_ref, w1_ref, w2_ref, hs_ref, hl_ref, h_s, hb_s):
    i = pl.program_id(0)
    j = lax.rem(i, tiles)

    @pl.when(i == 0)
    def _():
        h_s[...] = x_ref[...].astype(F32)

    @pl.when(j == 0)
    def _():
        hb_s[...] = h_s[...].astype(BF)
        hs_ref[0] = hb_s[...]

    z = dot(hb_s[...], w1_ref[0].astype(BF))
    h_s[...] += dot(gelu(z).astype(BF), w2_ref[0].astype(BF))

    @pl.when(i == LAYERS * tiles - 1)
    def _():
        hl_ref[...] = h_s[...]


def forward_first(x, w_in, w_out):
    tiles = 2
    th = HID // tiles
    full = pl.BlockSpec((ROWS, DIM), lambda i: (0, 0))
    return pl.pallas_call(
        functools.partial(fwd_kernel, tiles),
        grid=(LAYERS * tiles,),
        in_specs=[
            full,
            pl.BlockSpec((1, DIM, th), lambda i: (i // tiles, 0, i % tiles)),
            pl.BlockSpec((1, th, DIM), lambda i: (i // tiles, i % tiles, 0)),
        ],
        out_specs=[pl.BlockSpec((1, ROWS, DIM), lambda i: (i // tiles, 0, 0)), full],
        out_shape=[
            jax.ShapeDtypeStruct((LAYERS, ROWS, DIM), BF),
            jax.ShapeDtypeStruct((ROWS, DIM), F32),
        ],
        scratch_shapes=[pltpu.VMEM((ROWS, DIM), F32), pltpu.VMEM((ROWS, DIM), BF)],
        compiler_params=pltpu.CompilerParams(vmem_limit_bytes=VMEM_LIMIT),
        name="fwd_first",
    )(x, w_in, w_out)


def bwd_kernel(
    inv, w1_ref, w2_ref, hb_ref, hl_ref, y_ref, out_ref,
    e_s, eb_s, ht_s, gst, rb, acc, rv1, rv2, rv3,
    s0, r0, s1, r1, s2, r2, s3, r3,
):
    i = pl.program_id(0)
    me = lax.axis_index("data")
    core = lax.rem(me, 2)
    sib = me + 1 - 2 * core

    @pl.when(i == 0)
    def _():
        bar = pltpu.get_barrier_semaphore()
        pl.semaphore_signal(bar, inc=1, device_id=(sib,), device_id_type=MESH)
        for a in range(3):
            pl.semaphore_signal(bar, inc=1, device_id=(axis_peer(me, a)[1],), device_id_type=MESH)
        pl.semaphore_wait(bar, 4)

    def core_copy(u):
        return pltpu.make_async_remote_copy(
            src_ref=gst.at[lax.rem(u, 4), 1 - core], dst_ref=rb.at[lax.rem(u, RING)],
            send_sem=s0.at[lax.rem(u, 4)], recv_sem=r0.at[lax.rem(u, RING)],
            device_id=(sib,), device_id_type=MESH)

    def geometry(u, k):
        rot = lax.rem(u, 3)
        peers = [axis_peer(me, lax.rem(rot + k + p, 3)) for p in range(3)]
        return [b for b, _ in peers], [n for _, n in peers]

    def rows_of(k, bit):
        return pl.ds(pl.multiple_of(START[k] + bit * HALF[k], 16), HALF[k])

    def cols_of(start, size):
        return pl.ds(pl.multiple_of(start, 128), size)

    def stage_copy(u, k, p):
        bits, peers = geometry(u, k)
        slot = lax.rem(u, RING)
        hs = pl.ds(HSTART[k], HALF[k])
        if p == 0:
            src, dst = acc.at[slot, rows_of(k, 1 - bits[0])], rv1.at[slot, hs]
        elif p == 1:
            src, dst = acc.at[slot, rows_of(k, bits[0]), cols_of((1 - bits[1]) * 256, 256)], rv2.at[slot, hs]
        else:
            src = acc.at[slot, rows_of(k, bits[0]), cols_of(bits[1] * 256 + (1 - bits[2]) * 128, 128)]
            dst = rv3.at[slot, hs]
        ss, rs = ((s1, r1), (s2, r2), (s3, r3))[p]
        return pltpu.make_async_remote_copy(
            src_ref=src, dst_ref=dst, send_sem=ss.at[lax.rem(u, 4), k], recv_sem=rs.at[slot, k],
            device_id=(peers[p],), device_id_type=MESH)

    def add(a, b):
        return (a.astype(F32) + b.astype(F32)).astype(BF)

    @pl.when(i >= 8)
    def _():
        u = i - 8
        slot = lax.rem(u, RING)
        for k in range(3):
            stage_copy(u, k, 2).wait()
        for k in range(3):
            bits, _ = geometry(u, k)
            hs = pl.ds(HSTART[k], HALF[k])
            out_ref[0, hs, :] = add(acc[slot, rows_of(k, bits[0]), cols_of(bits[1] * 256 + bits[2] * 128, 128)], rv3[slot, hs, :])

    @pl.when((i >= 6) & (i < UNITS + 6))
    def _():
        u = i - 6
        slot = lax.rem(u, RING)
        for k in range(3):
            stage_copy(u, k, 1).wait()
        for k in range(3):
            bits, _ = geometry(u, k)
            hs = pl.ds(HSTART[k], HALF[k])
            idx = (slot, rows_of(k, bits[0]), cols_of(bits[1] * 256, 256))
            acc[idx] = add(acc[idx], rv2[slot, hs, :])
        for k in range(3):
            stage_copy(u, k, 2).start()

    @pl.when((i >= 4) & (i < UNITS + 4))
    def _():
        u = i - 4
        slot = lax.rem(u, RING)
        for k in range(3):
            stage_copy(u, k, 0).wait()
        for k in range(3):
            bits, _ = geometry(u, k)
            hs = pl.ds(HSTART[k], HALF[k])
            idx = (slot, rows_of(k, bits[0]), pl.ds(0, DIM))
            acc[idx] = add(acc[idx], rv1[slot, hs, :])
        for k in range(3):
            stage_copy(u, k, 1).start()

    @pl.when((i >= 2) & (i < UNITS + 2))
    def _():
        u = i - 2
        slot = lax.rem(u, RING)
        core_copy(u).wait()
        acc[slot] = add(gst[lax.rem(u, 4), core], rb[slot])
        for k in range(3):
            stage_copy(u, k, 0).start()

    @pl.when(i == 0)
    def _():
        e_s[...] = (hl_ref[...] - y_ref[...].astype(F32)) * inv

    @pl.when(i < UNITS)
    def _():
        @pl.when(lax.rem(i, PER) == 0)
        def _():
            eb_s[...] = e_s[...].astype(BF)
            ht_s[...] = hb_ref[0].T

        g = lax.rem(i, 4)
        eb = eb_s[...]
        w1 = w1_ref[0].astype(BF)
        w2 = w2_ref[0].astype(BF)
        z = dot(hb_ref[0], w1)
        q = dot(eb, w2, 1, 1)
        a, da = gelu_both(z)
        s = (da * q).astype(BF)
        gst[g, 1] = dot(a.astype(BF).T, eb).astype(BF)
        gst[g, 0] = dot(ht_s[...], s).astype(BF)
        e_s[...] += dot(s, w1, 1, 1)
        core_copy(i).start()


def backward_scatter(w_in, w_out, hs, hl, y, inv):
    last = UNITS - 1

    def layer(i):
        return LAYERS - 1 - jnp.minimum(i, last) // PER

    full = pl.BlockSpec((ROWS, DIM), lambda i: (0, 0))
    dma = pltpu.SemaphoreType.DMA
    return pl.pallas_call(
        functools.partial(bwd_kernel, inv),
        grid=(UNITS + 8,),
        in_specs=[
            pl.BlockSpec((1, DIM, TILE), lambda i: (layer(i), 0, jnp.minimum(i, last) % PER)),
            pl.BlockSpec((1, TILE, DIM), lambda i: (layer(i), jnp.minimum(i, last) % PER, 0)),
            pl.BlockSpec((1, ROWS, DIM), lambda i: (layer(i), 0, 0)),
            full, full,
        ],
        out_specs=pl.BlockSpec((1, 256, 128), lambda i: (jnp.maximum(i - 8, 0), 0, 0)),
        out_shape=jax.ShapeDtypeStruct((UNITS, 256, 128), BF),
        scratch_shapes=[
            pltpu.VMEM((ROWS, DIM), F32), pltpu.VMEM((ROWS, DIM), BF), pltpu.VMEM((DIM, ROWS), BF),
            pltpu.VMEM((4, 2, 512, 512), BF), pltpu.VMEM((RING, 512, 512), BF), pltpu.VMEM((RING, 512, 512), BF),
            pltpu.VMEM((RING, 256, 512), BF), pltpu.VMEM((RING, 256, 256), BF), pltpu.VMEM((RING, 256, 128), BF),
            dma((4,)), dma((RING,)), dma((4, 3)), dma((RING, 3)), dma((4, 3)), dma((RING, 3)), dma((4, 3)), dma((RING, 3)),
        ],
        compiler_params=pltpu.CompilerParams(
            vmem_limit_bytes=VMEM_LIMIT, collective_id=0, has_side_effects=True),
        name="bwd_scatter",
    )(w_in, w_out, hs, hl, y)


def upd_kernel(lo, hi, nalias, h_ref, g_ref, w1_ref, w2_ref, m1_ref, m2_ref, *rest):
    w1o, w2o, m1o, m2o, ho_ref, h_s, hb_s = rest[nalias:]
    i = pl.program_id(0)
    layer = lo + i // PER
    rot = lax.rem((LAYERS - 1 - layer) * PER + lax.rem(i, PER), 3)

    @pl.when(i == 0)
    def _():
        h_s[...] = h_ref[...].astype(F32)

    @pl.when(lax.rem(i, PER) == 0)
    def _():
        hb_s[...] = h_s[...].astype(BF)

    def chip(q, _):
        for k in range(3):
            bits = []
            for p in range(3):
                a = lax.rem(rot + k + p, 3)
                stride = lax.div(a * a + a + 2, 2)
                bits.append(lax.rem(lax.div(q, stride), 2))
            rows = pl.ds(pl.multiple_of(START[k] + bits[0] * HALF[k], 16), HALF[k])
            cols = pl.ds(pl.multiple_of(bits[1] * 256 + bits[2] * 128, 128), 128)
            for c, (w, m, wo, mo) in enumerate(((w1_ref, m1_ref, w1o, m1o), (w2_ref, m2_ref, w2o, m2o))):
                g = g_ref[2 * q + c, 0, pl.ds(HSTART[k], HALF[k]), :].astype(F32)
                mn = MU * m[0, rows, cols] + g
                mo[0, rows, cols] = mn
                wo[0, rows, cols] = w[0, rows, cols] - STEP * mn
        return 0

    lax.fori_loop(0, 8, chip, 0)
    z = dot(hb_s[...], w1o[0].astype(BF))
    h_s[...] += dot(gelu(z).astype(BF), w2o[0].astype(BF))

    @pl.when(i == (hi - lo) * PER - 1)
    def _():
        ho_ref[...] = h_s[...]


def update_forward(lo, hi, h, g, weights, prev):
    n = (hi - lo) * PER

    def in_map(i):
        return (lo + i // PER, 0, i % PER)

    def out_map(i):
        return (lo + i // PER, i % PER, 0)

    b1 = pl.BlockSpec((1, DIM, TILE), in_map)
    b2 = pl.BlockSpec((1, TILE, DIM), out_map)
    full = pl.BlockSpec((ROWS, DIM), lambda i: (0, 0))
    gspec = pl.BlockSpec((16, 1, 256, 128), lambda i: (0, (hi - lo - 1 - i // PER) * PER + i % PER, 0, 0))
    nalias = len(prev)
    s1 = jax.ShapeDtypeStruct((LAYERS, DIM, HID), F32)
    s2 = jax.ShapeDtypeStruct((LAYERS, HID, DIM), F32)
    return pl.pallas_call(
        functools.partial(upd_kernel, lo, hi, nalias),
        grid=(n,),
        in_specs=[full, gspec, b1, b2, b1, b2] + [pl.BlockSpec(memory_space=pl.ANY)] * nalias,
        out_specs=[b1, b2, b1, b2, full],
        out_shape=[s1, s2, s1, s2, jax.ShapeDtypeStruct((ROWS, DIM), F32)],
        input_output_aliases={6 + a: a for a in range(nalias)},
        scratch_shapes=[pltpu.VMEM((ROWS, DIM), F32), pltpu.VMEM((ROWS, DIM), BF)],
        compiler_params=pltpu.CompilerParams(vmem_limit_bytes=VMEM_LIMIT),
        cost_estimate=pl.CostEstimate(flops=n * 4 * 512**3, bytes_accessed=n * 9 * 2**20, transcendentals=0),
        name="upd_fwd",
    )(h, g, *weights, *prev)


def solution(mesh):
    groups = mesh.shape["data"]
    rows_spec = P("data", None)

    def local_steps(w_in, w_out, mom_in, mom_out, x_first, y_first, x_second, y_second):
        hs, hl = forward_first(x_first, w_in, w_out)
        shards = backward_scatter(w_in, w_out, hs, hl, y_first, 1.0 / (ROWS * groups * DIM))
        gathered = []
        for lo, hi in CHUNKS:
            part = shards[(LAYERS - hi) * PER:(LAYERS - lo) * PER]
            gathered.append(lax.all_gather(part, "data", axis=0, tiled=False))
        h, prev = x_second, ()
        for (lo, hi), g in zip(CHUNKS, gathered):
            *prev, h = update_forward(lo, hi, h, g, (w_in, w_out, mom_in, mom_out), tuple(prev))
        row_diff = h - y_second.astype(F32)
        loss_rows = jnp.sum(row_diff * row_diff, axis=-1) / (2 * DIM)
        return prev[0], prev[1], prev[2], prev[3], loss_rows, h

    return jax.shard_map(
        local_steps, mesh=mesh,
        in_specs=(P(), P(), P(), P(), rows_spec, rows_spec, rows_spec, rows_spec),
        out_specs=(P(), P(), P(), P(), P("data"), rows_spec), check_vma=False)
```

```python
import functools

import jax
import jax.numpy as jnp
from jax import lax
from jax.experimental import pallas as pl
from jax.experimental.pallas import tpu as pltpu
from jax.sharding import PartitionSpec as P

MESH = pl.DeviceIdType.MESH
BF = jnp.bfloat16
F32 = jnp.float32
LAYERS, DIM, HID, ROWS = 16, 512, 2048, 512
TILE = 512
PER = HID // TILE
UNITS = LAYERS * PER
STEP = 1.0 / LAYERS
MU = 0.9
C0 = 0.7978845608028654
C1 = C0 * 0.044715
BLOCK = (160, 160, 192)
START = (0, 160, 320)
HALF = (80, 80, 96)
HSTART = (0, 80, 160)
RING = 8
ARING = 16
DEPTH = 18
CHUNKS = ((0, 6), (6, 11), (11, 14), (14, 16))
SPANS = tuple(((LAYERS - hi) * PER, (hi - lo) * PER) for lo, hi in CHUNKS)
SUB = 2
VMEM_LIMIT = 62 * 2**20


def dot(a, b, ca=1, cb=0):
    return lax.dot_general(a, b, (((ca,), (cb,)), ((), ())), preferred_element_type=F32)


def gelu(z):
    t = jnp.tanh(z * (C0 + C1 * (z * z)))
    return z * (0.5 * t + 0.5)


def gelu_both(z):
    z2 = z * z
    t = jnp.tanh(z * (C0 + C1 * z2))
    cdf = 0.5 * t + 0.5
    return z * cdf, cdf + (0.5 * z) * ((1.0 - t * t) * (C0 + (3.0 * C1) * z2))


def axis_peer(me, order):
    stride = order * order + order + 2
    bit = lax.rem(lax.div(me, stride), 2)
    return bit, me + (1 - 2 * bit) * stride


def fwd_kernel(tiles, x_ref, w1_ref, w2_ref, hs_ref, hl_ref, h_s, hb_s):
    i = pl.program_id(0)
    j = lax.rem(i, tiles)

    @pl.when(i == 0)
    def _():
        h_s[...] = x_ref[...].astype(F32)

    @pl.when(j == 0)
    def _():
        hb_s[...] = h_s[...].astype(BF)
        hs_ref[0] = hb_s[...]

    z = dot(hb_s[...], w1_ref[0].astype(BF))
    h_s[...] += dot(gelu(z).astype(BF), w2_ref[0].astype(BF))

    @pl.when(i == LAYERS * tiles - 1)
    def _():
        hl_ref[...] = h_s[...]


def forward_first(x, w_in, w_out):
    tiles = 1
    th = HID // tiles
    full = pl.BlockSpec((ROWS, DIM), lambda i: (0, 0))
    return pl.pallas_call(
        functools.partial(fwd_kernel, tiles),
        grid=(LAYERS * tiles,),
        in_specs=[
            full,
            pl.BlockSpec((1, DIM, th), lambda i: (i // tiles, 0, i % tiles)),
            pl.BlockSpec((1, th, DIM), lambda i: (i // tiles, i % tiles, 0)),
        ],
        out_specs=[pl.BlockSpec((1, ROWS, DIM), lambda i: (i // tiles, 0, 0)), full],
        out_shape=[
            jax.ShapeDtypeStruct((LAYERS, ROWS, DIM), BF),
            jax.ShapeDtypeStruct((ROWS, DIM), F32),
        ],
        scratch_shapes=[pltpu.VMEM((ROWS, DIM), F32), pltpu.VMEM((ROWS, DIM), BF)],
        compiler_params=pltpu.CompilerParams(vmem_limit_bytes=VMEM_LIMIT),
        name="fwd_first",
    )(x, w_in, w_out)


def bwd_kernel(
    inv, w1_ref, w2_ref, hb_ref, hl_ref, y_ref, *rest,
):
    full_ref, out_refs, (
        e_s, eb_s, ht_s, gst, rb, acc, gb, rv1, rv2, rv3, tv3,
        s0, r0, s1, r1, s2, r2, s3, r3,
        ts0, tr0, ts1, tr1, ts2, tr2, ts3, tr3, ls,
    ) = rest[0], rest[1:len(CHUNKS)], rest[len(CHUNKS):]
    whole = SPANS[0][0]
    i = pl.program_id(0)
    me = lax.axis_index("data")
    core = lax.rem(me, 2)
    sib = me + 1 - 2 * core

    @pl.when(i == 0)
    def _():
        bar = pltpu.get_barrier_semaphore()
        pl.semaphore_signal(bar, inc=1, device_id=(sib,), device_id_type=MESH)
        for a in range(3):
            pl.semaphore_signal(bar, inc=1, device_id=(axis_peer(me, a)[1],), device_id_type=MESH)
        pl.semaphore_wait(bar, 4)

    def core_copy(u):
        return pltpu.make_async_remote_copy(
            src_ref=gst.at[lax.rem(u, 4), 1 - core], dst_ref=rb.at[lax.rem(u, RING)],
            send_sem=s0.at[lax.rem(u, 4)], recv_sem=r0.at[lax.rem(u, RING)],
            device_id=(sib,), device_id_type=MESH)

    def geometry(u, k):
        rot = lax.rem(u, 3)
        peers = [axis_peer(me, lax.rem(rot + k + p, 3)) for p in range(3)]
        return [b for b, _ in peers], [n for _, n in peers]

    def rows_of(k, bit):
        return pl.ds(pl.multiple_of(START[k] + bit * HALF[k], 16), HALF[k])

    def cols_of(start, size):
        return pl.ds(pl.multiple_of(start, 128), size)

    def stage_copy(u, k, p):
        bits, peers = geometry(u, k)
        slot, aslot = lax.rem(u, RING), lax.rem(u, ARING)
        hs = pl.ds(HSTART[k], HALF[k])
        if p == 0:
            src, dst = acc.at[aslot, rows_of(k, 1 - bits[0])], rv1.at[slot, hs]
        elif p == 1:
            src, dst = acc.at[aslot, rows_of(k, bits[0]), cols_of((1 - bits[1]) * 256, 256)], rv2.at[slot, hs]
        else:
            src = acc.at[aslot, rows_of(k, bits[0]), cols_of(bits[1] * 256 + (1 - bits[2]) * 128, 128)]
            dst = rv3.at[slot, hs]
        ss, rs = ((s1, r1), (s2, r2), (s3, r3))[p]
        return pltpu.make_async_remote_copy(
            src_ref=src, dst_ref=dst, send_sem=ss.at[lax.rem(u, 4), k], recv_sem=rs.at[slot, k],
            device_id=(peers[p],), device_id_type=MESH)

    def gather_copy(u, k, p):
        bits, peers = geometry(u, k)
        cols = (pl.ds(0, DIM), cols_of(bits[1] * 256, 256), cols_of(bits[1] * 256 + bits[2] * 128, 128))[p]
        part = acc.at[lax.rem(u, ARING), rows_of(k, bits[0]), cols]
        into = tv3.at[lax.rem(u, RING), pl.ds(HSTART[k], HALF[k])] if p == 2 else part
        ss, rs = ((ts1, tr1), (ts2, tr2), (ts3, tr3))[p]
        return pltpu.make_async_remote_copy(
            src_ref=part, dst_ref=into, send_sem=ss.at[lax.rem(u, 4), k], recv_sem=rs.at[lax.rem(u, RING), k],
            device_id=(peers[p],), device_id_type=MESH)

    def gather_core(u):
        return pltpu.make_async_remote_copy(
            src_ref=acc.at[lax.rem(u, ARING)], dst_ref=gb.at[lax.rem(u, RING)],
            send_sem=ts0.at[lax.rem(u, 4)], recv_sem=tr0.at[lax.rem(u, RING)],
            device_id=(sib,), device_id_type=MESH)

    def store_copies(u):
        n, j = u - whole, lax.rem(u, 4)
        return (pltpu.make_async_copy(acc.at[lax.rem(u, ARING)], full_ref.at[n, core], ls.at[j, 0]),
                pltpu.make_async_copy(gb.at[lax.rem(u, RING)], full_ref.at[n, 1 - core], ls.at[j, 1]))

    def add(a, b):
        return (a.astype(F32) + b.astype(F32)).astype(BF)

    def gathering(lag):
        return (i >= whole + lag) & (i < UNITS + lag)

    @pl.when(gathering(18))
    def _():
        for c in store_copies(i - 18):
            c.wait()

    @pl.when(gathering(16))
    def _():
        gather_core(i - 16).wait()
        for c in store_copies(i - 16):
            c.start()

    @pl.when(gathering(14))
    def _():
        for k in range(3):
            gather_copy(i - 14, k, 0).wait()
        gather_core(i - 14).start()

    @pl.when(gathering(12))
    def _():
        for k in range(3):
            gather_copy(i - 12, k, 1).wait()
        for k in range(3):
            gather_copy(i - 12, k, 0).start()

    @pl.when(gathering(10))
    def _():
        u = i - 10
        for k in range(3):
            gather_copy(u, k, 2).wait()
        for k in range(3):
            bits, _ = geometry(u, k)
            cols = cols_of(bits[1] * 256 + (1 - bits[2]) * 128, 128)
            acc[lax.rem(u, ARING), rows_of(k, bits[0]), cols] = tv3[lax.rem(u, RING), pl.ds(HSTART[k], HALF[k]), :]
        for k in range(3):
            gather_copy(u, k, 1).start()

    @pl.when((i >= 8) & (i < UNITS + 8))
    def _():
        u = i - 8
        slot, aslot = lax.rem(u, RING), lax.rem(u, ARING)
        for k in range(3):
            stage_copy(u, k, 2).wait()
        for k in range(3):
            bits, _ = geometry(u, k)
            hs = pl.ds(HSTART[k], HALF[k])
            idx = (aslot, rows_of(k, bits[0]), cols_of(bits[1] * 256 + bits[2] * 128, 128))
            done = add(acc[idx], rv3[slot, hs, :])

            @pl.when(u >= whole)
            def _():
                acc[idx] = done
                gather_copy(u, k, 2).start()

            for (first, count), out_ref in zip(SPANS[1:], out_refs):
                @pl.when((u >= first) & (u < first + count))
                def _(out_ref=out_ref):
                    out_ref[0, hs, :] = done

    @pl.when((i >= 6) & (i < UNITS + 6))
    def _():
        u = i - 6
        slot, aslot = lax.rem(u, RING), lax.rem(u, ARING)
        for k in range(3):
            stage_copy(u, k, 1).wait()
        for k in range(3):
            bits, _ = geometry(u, k)
            hs = pl.ds(HSTART[k], HALF[k])
            idx = (aslot, rows_of(k, bits[0]), cols_of(bits[1] * 256, 256))
            acc[idx] = add(acc[idx], rv2[slot, hs, :])
        for k in range(3):
            stage_copy(u, k, 2).start()

    @pl.when((i >= 4) & (i < UNITS + 4))
    def _():
        u = i - 4
        slot, aslot = lax.rem(u, RING), lax.rem(u, ARING)
        for k in range(3):
            stage_copy(u, k, 0).wait()
        for k in range(3):
            bits, _ = geometry(u, k)
            hs = pl.ds(HSTART[k], HALF[k])
            idx = (aslot, rows_of(k, bits[0]), pl.ds(0, DIM))
            acc[idx] = add(acc[idx], rv1[slot, hs, :])
        for k in range(3):
            stage_copy(u, k, 1).start()

    @pl.when((i >= 2) & (i < UNITS + 2))
    def _():
        u = i - 2
        slot, aslot = lax.rem(u, RING), lax.rem(u, ARING)
        core_copy(u).wait()
        acc[aslot] = add(gst[lax.rem(u, 4), core], rb[slot])
        for k in range(3):
            stage_copy(u, k, 0).start()

    @pl.when(i == 0)
    def _():
        e_s[...] = (hl_ref[...] - y_ref[...].astype(F32)) * inv

    @pl.when(i < UNITS)
    def _():
        @pl.when(lax.rem(i, PER) == 0)
        def _():
            eb_s[...] = e_s[...].astype(BF)
            ht_s[...] = hb_ref[0].T

        g = lax.rem(i, 4)
        eb = eb_s[...]
        w1 = w1_ref[0].astype(BF)
        w2 = w2_ref[0].astype(BF)
        z = dot(hb_ref[0], w1)
        q = dot(eb, w2, 1, 1)
        a, da = gelu_both(z)
        s = (da * q).astype(BF)
        gst[g, 1] = dot(a.astype(BF).T, eb).astype(BF)
        gst[g, 0] = dot(ht_s[...], s).astype(BF)
        e_s[...] += dot(s, w1, 1, 1)
        core_copy(i).start()


def shard_map_of(first, count, i):
    return jnp.clip(i - 8 - first, 0, count - 1), 0, 0


def backward_scatter(w_in, w_out, hs, hl, y, inv):
    last = UNITS - 1

    def layer(i):
        return LAYERS - 1 - jnp.minimum(i, last) // PER

    full = pl.BlockSpec((ROWS, DIM), lambda i: (0, 0))
    dma = pltpu.SemaphoreType.DMA
    return pl.pallas_call(
        functools.partial(bwd_kernel, inv),
        grid=(UNITS + DEPTH,),
        in_specs=[
            pl.BlockSpec((1, DIM, TILE), lambda i: (layer(i), 0, jnp.minimum(i, last) % PER)),
            pl.BlockSpec((1, TILE, DIM), lambda i: (layer(i), jnp.minimum(i, last) % PER, 0)),
            pl.BlockSpec((1, ROWS, DIM), lambda i: (layer(i), 0, 0)),
            full, full,
        ],
        out_specs=[pl.BlockSpec(memory_space=pl.ANY)] + [
            pl.BlockSpec((1, 256, 128), functools.partial(shard_map_of, f, n)) for f, n in SPANS[1:]],
        out_shape=[jax.ShapeDtypeStruct((SPANS[0][1], 2, 512, 512), BF)] + [
            jax.ShapeDtypeStruct((n, 256, 128), BF) for _, n in SPANS[1:]],
        scratch_shapes=[
            pltpu.VMEM((ROWS, DIM), F32), pltpu.VMEM((ROWS, DIM), BF), pltpu.VMEM((DIM, ROWS), BF),
            pltpu.VMEM((4, 2, 512, 512), BF), pltpu.VMEM((RING, 512, 512), BF), pltpu.VMEM((ARING, 512, 512), BF),
            pltpu.VMEM((RING, 512, 512), BF),
            pltpu.VMEM((RING, 256, 512), BF), pltpu.VMEM((RING, 256, 256), BF), pltpu.VMEM((RING, 256, 128), BF),
            pltpu.VMEM((RING, 256, 128), BF),
        ] + [dma(n) for n in ((4,), (RING,)) + ((4, 3), (RING, 3)) * 3] * 2 + [dma((4, 2))],
        compiler_params=pltpu.CompilerParams(
            vmem_limit_bytes=VMEM_LIMIT, collective_id=0, has_side_effects=True),
        name="bwd_scatter",
    )(w_in, w_out, hs, hl, y)


def upd_kernel(lo, hi, nalias, h_ref, g_ref, w1_ref, w2_ref, m1_ref, m2_ref, *rest):
    w1o, w2o, m1o, m2o, ho_ref, h_s, hb_s, wb1, wb2 = rest[nalias:]
    i = pl.program_id(0)
    steps = PER // SUB
    layer = lo + i // steps

    @pl.when(i == 0)
    def _():
        h_s[...] = h_ref[...].astype(F32)

    @pl.when(lax.rem(i, steps) == 0)
    def _():
        hb_s[...] = h_s[...].astype(BF)

    def chip(q, t, rot):
        for k in range(3):
            bits = []
            for p in range(3):
                a = lax.rem(rot + k + p, 3)
                stride = lax.div(a * a + a + 2, 2)
                bits.append(lax.rem(lax.div(q, stride), 2))
            row = START[k] + bits[0] * HALF[k]
            col = bits[1] * 256 + bits[2] * 128
            for c, (w, m, wo, mo, wb) in enumerate(((w1_ref, m1_ref, w1o, m1o, wb1), (w2_ref, m2_ref, w2o, m2o, wb2))):
                rows = pl.ds(pl.multiple_of(row + c * t * TILE, 16), HALF[k])
                cols = pl.ds(pl.multiple_of(col + (1 - c) * t * TILE, 128), 128)
                g = g_ref[2 * q + c, t, pl.ds(HSTART[k], HALF[k]), :].astype(F32)
                mn = MU * m[0, rows, cols] + g
                wn = w[0, rows, cols] - STEP * mn
                mo[0, rows, cols] = mn
                wo[0, rows, cols] = wn
                wb[rows, cols] = wn.astype(BF)

    for t in range(SUB):
        rot = lax.rem((LAYERS - 1 - layer) * PER + lax.rem(i, steps) * SUB + t, 3)

        def body(q, _, t=t, rot=rot):
            chip(q, t, rot)
            return 0

        def rows_body(r, _, t=t):
            for c, (w, m, wo, mo, wb) in enumerate(((w1_ref, m1_ref, w1o, m1o, wb1), (w2_ref, m2_ref, w2o, m2o, wb2))):
                rows = pl.ds(pl.multiple_of(r * 32 + c * t * TILE, 32), 32)
                cols = pl.ds((1 - c) * t * TILE, TILE)
                mn = MU * m[0, rows, cols] + g_ref[t, c, pl.ds(pl.multiple_of(r * 32, 32), 32), :].astype(F32)
                wn = w[0, rows, cols] - STEP * mn
                mo[0, rows, cols] = mn
                wo[0, rows, cols] = wn
                wb[rows, cols] = wn.astype(BF)
            return 0

        if lo == 0:
            lax.fori_loop(0, 16, rows_body, 0, unroll=2)
        else:
            lax.fori_loop(0, 8, body, 0, unroll=2)
    z = dot(hb_s[...], wb1[...])
    h_s[...] += dot(gelu(z).astype(BF), wb2[...])

    @pl.when(i == (hi - lo) * steps - 1)
    def _():
        ho_ref[...] = h_s[...]


def update_forward(lo, hi, h, g, weights, prev):
    steps = PER // SUB
    n = (hi - lo) * steps
    wide = SUB * TILE
    b1 = pl.BlockSpec((1, DIM, wide), lambda i: (lo + i // steps, 0, i % steps))
    b2 = pl.BlockSpec((1, wide, DIM), lambda i: (lo + i // steps, i % steps, 0))
    full = pl.BlockSpec((ROWS, DIM), lambda i: (0, 0))
    def order(i):
        return (hi - lo - 1 - i // steps) * steps + i % steps

    if lo == 0:
        gspec = pl.BlockSpec((SUB, 2, 512, 512), lambda i: (order(i), 0, 0, 0))
    else:
        gspec = pl.BlockSpec((16, SUB, 256, 128), lambda i: (0, order(i), 0, 0))
    nalias = len(prev)
    s1 = jax.ShapeDtypeStruct((LAYERS, DIM, HID), F32)
    s2 = jax.ShapeDtypeStruct((LAYERS, HID, DIM), F32)
    return pl.pallas_call(
        functools.partial(upd_kernel, lo, hi, nalias),
        grid=(n,),
        in_specs=[full, gspec, b1, b2, b1, b2] + [pl.BlockSpec(memory_space=pl.ANY)] * nalias,
        out_specs=[b1, b2, b1, b2, full],
        out_shape=[s1, s2, s1, s2, jax.ShapeDtypeStruct((ROWS, DIM), F32)],
        input_output_aliases={6 + a: a for a in range(nalias)},
        scratch_shapes=[
            pltpu.VMEM((ROWS, DIM), F32), pltpu.VMEM((ROWS, DIM), BF),
            pltpu.VMEM((DIM, wide), BF), pltpu.VMEM((wide, DIM), BF)],
        compiler_params=pltpu.CompilerParams(vmem_limit_bytes=VMEM_LIMIT),
        cost_estimate=pl.CostEstimate(flops=n * SUB * 4 * 512**3, bytes_accessed=n * SUB * 9 * 2**20, transcendentals=0),
        name="upd_fwd",
    )(h, g, *weights, *prev)


def solution(mesh):
    groups = mesh.shape["data"]
    rows_spec = P("data", None)

    def local_steps(w_in, w_out, mom_in, mom_out, x_first, y_first, x_second, y_second):
        hs, hl = forward_first(x_first, w_in, w_out)
        first, *shards = backward_scatter(w_in, w_out, hs, hl, y_first, 1.0 / (ROWS * groups * DIM))
        gathered = [first] + [lax.all_gather(part, "data", axis=0, tiled=False) for part in shards]
        h, prev = x_second, ()
        for (lo, hi), g in zip(CHUNKS, gathered):
            *prev, h = update_forward(lo, hi, h, g, (w_in, w_out, mom_in, mom_out), tuple(prev))
        row_diff = h - y_second.astype(F32)
        loss_rows = jnp.sum(row_diff * row_diff, axis=-1) / (2 * DIM)
        return prev[0], prev[1], prev[2], prev[3], loss_rows, h

    return jax.shard_map(
        local_steps, mesh=mesh,
        in_specs=(P(), P(), P(), P(), rows_spec, rows_spec, rows_spec, rows_spec),
        out_specs=(P(), P(), P(), P(), P("data"), rows_spec), check_vma=False)
```

```python
import functools

import jax
import jax.numpy as jnp
from jax import lax
from jax.experimental import pallas as pl
from jax.experimental.pallas import tpu as pltpu
from jax.sharding import PartitionSpec as P

MESH = pl.DeviceIdType.MESH
BF = jnp.bfloat16
F32 = jnp.float32
LAYERS, DIM, HID, ROWS = 16, 512, 2048, 512
TILE = 512
PER = HID // TILE
UNITS = LAYERS * PER
STEP = 1.0 / LAYERS
MU = 0.9
C0 = 0.7978845608028654
C1 = C0 * 0.044715
BLOCK = (160, 160, 192)
START = (0, 160, 320)
HALF = (80, 80, 96)
HSTART = (0, 80, 160)
RING = 8
ARING = 16
DEPTH = 18
CHUNKS = ((0, 7), (7, 12), (12, 15), (15, 16))
AHEAD = 4
SLOTS = 8
SPANS = tuple(((LAYERS - hi) * PER, (hi - lo) * PER) for lo, hi in CHUNKS)
VMEM_LIMIT = 62 * 2**20


def dot(a, b, ca=1, cb=0):
    return lax.dot_general(a, b, (((ca,), (cb,)), ((), ())), preferred_element_type=F32)


def gelu(z):
    t = jnp.tanh(z * (C0 + C1 * (z * z)))
    return z * (0.5 * t + 0.5)


def gelu_both(z):
    z2 = z * z
    t = jnp.tanh(z * (C0 + C1 * z2))
    cdf = 0.5 * t + 0.5
    return z * cdf, cdf + (0.5 * z) * ((1.0 - t * t) * (C0 + (3.0 * C1) * z2))


def axis_peer(me, order):
    stride = order * order + order + 2
    bit = lax.rem(lax.div(me, stride), 2)
    return bit, me + (1 - 2 * bit) * stride


def fwd_kernel(x_ref, w1_hbm, w2_hbm, hs_ref, hl_ref, h_s, hb_s, w1_s, w2_s, sem):
    i = pl.program_id(0)

    def load(layer, c):
        slot = lax.rem(layer, 3)
        src, dst = ((w1_hbm, w1_s), (w2_hbm, w2_s))[c]
        return pltpu.make_async_copy(src.at[layer], dst.at[slot], sem.at[slot, c])

    @pl.when(i == 0)
    def _():
        for c in range(2):
            load(0, c).start()
        h_s[...] = x_ref[...].astype(F32)

    hb_s[...] = h_s[...].astype(BF)
    hs_ref[0] = hb_s[...]
    slot = lax.rem(i, 3)
    load(i, 0).wait()

    @pl.when(i == 0)
    def _():
        for c in range(2):
            load(1, c).start()

    @pl.when(i + 2 < LAYERS)
    def _():
        for c in range(2):
            load(i + 2, c).start()

    z = dot(hb_s[...], w1_s[slot].astype(BF))
    load(i, 1).wait()
    h_s[...] += dot(gelu(z).astype(BF), w2_s[slot].astype(BF))

    @pl.when(i == LAYERS - 1)
    def _():
        hl_ref[...] = h_s[...]


def forward_first(x, w_in, w_out):
    full = pl.BlockSpec((ROWS, DIM), lambda i: (0, 0))
    hbm = pl.BlockSpec(memory_space=pl.ANY)
    return pl.pallas_call(
        fwd_kernel,
        grid=(LAYERS,),
        in_specs=[full, hbm, hbm],
        out_specs=[pl.BlockSpec((1, ROWS, DIM), lambda i: (i, 0, 0)), full],
        out_shape=[
            jax.ShapeDtypeStruct((LAYERS, ROWS, DIM), BF),
            jax.ShapeDtypeStruct((ROWS, DIM), F32),
        ],
        scratch_shapes=[
            pltpu.VMEM((ROWS, DIM), F32), pltpu.VMEM((ROWS, DIM), BF),
            pltpu.VMEM((3, DIM, HID), F32), pltpu.VMEM((3, HID, DIM), F32),
            pltpu.SemaphoreType.DMA((3, 2))],
        compiler_params=pltpu.CompilerParams(vmem_limit_bytes=VMEM_LIMIT),
        name="fwd_first",
    )(x, w_in, w_out)


def bwd_kernel(
    inv, w1_ref, w2_ref, hb_ref, hl_ref, y_ref, *rest,
):
    full_ref, out_refs, (
        e_s, eb_s, ht_s, gst, rb, acc, gb, rv1, rv2, rv3, tv3,
        s0, r0, s1, r1, s2, r2, s3, r3,
        ts0, tr0, ts1, tr1, ts2, tr2, ts3, tr3, ls,
    ) = rest[0], rest[1:len(CHUNKS)], rest[len(CHUNKS):]
    whole = SPANS[0][0]
    i = pl.program_id(0)
    me = lax.axis_index("data")
    core = lax.rem(me, 2)
    sib = me + 1 - 2 * core

    @pl.when(i == 0)
    def _():
        bar = pltpu.get_barrier_semaphore()
        pl.semaphore_signal(bar, inc=1, device_id=(sib,), device_id_type=MESH)
        for a in range(3):
            pl.semaphore_signal(bar, inc=1, device_id=(axis_peer(me, a)[1],), device_id_type=MESH)
        pl.semaphore_wait(bar, 4)

    def core_copy(u):
        return pltpu.make_async_remote_copy(
            src_ref=gst.at[lax.rem(u, 4), 1 - core], dst_ref=rb.at[lax.rem(u, RING)],
            send_sem=s0.at[lax.rem(u, 4)], recv_sem=r0.at[lax.rem(u, RING)],
            device_id=(sib,), device_id_type=MESH)

    def geometry(u, k):
        rot = lax.rem(u, 3)
        peers = [axis_peer(me, lax.rem(rot + k + p, 3)) for p in range(3)]
        return [b for b, _ in peers], [n for _, n in peers]

    def rows_of(k, bit):
        return pl.ds(pl.multiple_of(START[k] + bit * HALF[k], 16), HALF[k])

    def cols_of(start, size):
        return pl.ds(pl.multiple_of(start, 128), size)

    def stage_copy(u, k, p):
        bits, peers = geometry(u, k)
        slot, aslot = lax.rem(u, RING), lax.rem(u, ARING)
        hs = pl.ds(HSTART[k], HALF[k])
        if p == 0:
            src, dst = acc.at[aslot, rows_of(k, 1 - bits[0])], rv1.at[slot, hs]
        elif p == 1:
            src, dst = acc.at[aslot, rows_of(k, bits[0]), cols_of((1 - bits[1]) * 256, 256)], rv2.at[slot, hs]
        else:
            src = acc.at[aslot, rows_of(k, bits[0]), cols_of(bits[1] * 256 + (1 - bits[2]) * 128, 128)]
            dst = rv3.at[slot, hs]
        ss, rs = ((s1, r1), (s2, r2), (s3, r3))[p]
        return pltpu.make_async_remote_copy(
            src_ref=src, dst_ref=dst, send_sem=ss.at[lax.rem(u, 4), k], recv_sem=rs.at[slot, k],
            device_id=(peers[p],), device_id_type=MESH)

    def gather_copy(u, k, p):
        bits, peers = geometry(u, k)
        cols = (pl.ds(0, DIM), cols_of(bits[1] * 256, 256), cols_of(bits[1] * 256 + bits[2] * 128, 128))[p]
        part = acc.at[lax.rem(u, ARING), rows_of(k, bits[0]), cols]
        into = tv3.at[lax.rem(u, RING), pl.ds(HSTART[k], HALF[k])] if p == 2 else part
        ss, rs = ((ts1, tr1), (ts2, tr2), (ts3, tr3))[p]
        return pltpu.make_async_remote_copy(
            src_ref=part, dst_ref=into, send_sem=ss.at[lax.rem(u, 4), k], recv_sem=rs.at[lax.rem(u, RING), k],
            device_id=(peers[p],), device_id_type=MESH)

    def gather_core(u):
        return pltpu.make_async_remote_copy(
            src_ref=acc.at[lax.rem(u, ARING)], dst_ref=gb.at[lax.rem(u, RING)],
            send_sem=ts0.at[lax.rem(u, 4)], recv_sem=tr0.at[lax.rem(u, RING)],
            device_id=(sib,), device_id_type=MESH)

    def store_copies(u):
        n, j = u - whole, lax.rem(u, 4)
        return (pltpu.make_async_copy(acc.at[lax.rem(u, ARING)], full_ref.at[n, core], ls.at[j, 0]),
                pltpu.make_async_copy(gb.at[lax.rem(u, RING)], full_ref.at[n, 1 - core], ls.at[j, 1]))

    def add(a, b):
        return (a.astype(F32) + b.astype(F32)).astype(BF)

    def gathering(lag):
        return (i >= whole + lag) & (i < UNITS + lag)

    @pl.when(gathering(18))
    def _():
        for c in store_copies(i - 18):
            c.wait()

    @pl.when(gathering(16))
    def _():
        gather_core(i - 16).wait()
        for c in store_copies(i - 16):
            c.start()

    @pl.when(gathering(14))
    def _():
        for k in range(3):
            gather_copy(i - 14, k, 0).wait()
        gather_core(i - 14).start()

    @pl.when(gathering(12))
    def _():
        for k in range(3):
            gather_copy(i - 12, k, 1).wait()
        for k in range(3):
            gather_copy(i - 12, k, 0).start()

    @pl.when(gathering(10))
    def _():
        u = i - 10
        for k in range(3):
            gather_copy(u, k, 2).wait()
        for k in range(3):
            bits, _ = geometry(u, k)
            cols = cols_of(bits[1] * 256 + (1 - bits[2]) * 128, 128)
            acc[lax.rem(u, ARING), rows_of(k, bits[0]), cols] = tv3[lax.rem(u, RING), pl.ds(HSTART[k], HALF[k]), :]
        for k in range(3):
            gather_copy(u, k, 1).start()

    @pl.when((i >= 8) & (i < UNITS + 8))
    def _():
        u = i - 8
        slot, aslot = lax.rem(u, RING), lax.rem(u, ARING)
        for k in range(3):
            stage_copy(u, k, 2).wait()
        for k in range(3):
            bits, _ = geometry(u, k)
            hs = pl.ds(HSTART[k], HALF[k])
            idx = (aslot, rows_of(k, bits[0]), cols_of(bits[1] * 256 + bits[2] * 128, 128))
            done = add(acc[idx], rv3[slot, hs, :])

            @pl.when(u >= whole)
            def _():
                acc[idx] = done
                gather_copy(u, k, 2).start()

            for (first, count), out_ref in zip(SPANS[1:], out_refs):
                @pl.when((u >= first) & (u < first + count))
                def _(out_ref=out_ref):
                    out_ref[0, hs, :] = done

    @pl.when((i >= 6) & (i < UNITS + 6))
    def _():
        u = i - 6
        slot, aslot = lax.rem(u, RING), lax.rem(u, ARING)
        for k in range(3):
            stage_copy(u, k, 1).wait()
        for k in range(3):
            bits, _ = geometry(u, k)
            hs = pl.ds(HSTART[k], HALF[k])
            idx = (aslot, rows_of(k, bits[0]), cols_of(bits[1] * 256, 256))
            acc[idx] = add(acc[idx], rv2[slot, hs, :])
        for k in range(3):
            stage_copy(u, k, 2).start()

    @pl.when((i >= 4) & (i < UNITS + 4))
    def _():
        u = i - 4
        slot, aslot = lax.rem(u, RING), lax.rem(u, ARING)
        for k in range(3):
            stage_copy(u, k, 0).wait()
        for k in range(3):
            bits, _ = geometry(u, k)
            hs = pl.ds(HSTART[k], HALF[k])
            idx = (aslot, rows_of(k, bits[0]), pl.ds(0, DIM))
            acc[idx] = add(acc[idx], rv1[slot, hs, :])
        for k in range(3):
            stage_copy(u, k, 1).start()

    @pl.when((i >= 2) & (i < UNITS + 2))
    def _():
        u = i - 2
        slot, aslot = lax.rem(u, RING), lax.rem(u, ARING)
        core_copy(u).wait()
        acc[aslot] = add(gst[lax.rem(u, 4), core], rb[slot])
        for k in range(3):
            stage_copy(u, k, 0).start()

    @pl.when(i == 0)
    def _():
        e_s[...] = (hl_ref[...] - y_ref[...].astype(F32)) * inv

    @pl.when(i < UNITS)
    def _():
        @pl.when(lax.rem(i, PER) == 0)
        def _():
            eb_s[...] = e_s[...].astype(BF)
            ht_s[...] = hb_ref[0].T

        g = lax.rem(i, 4)
        eb = eb_s[...]
        w1 = w1_ref[0].astype(BF)
        w2 = w2_ref[0].astype(BF)
        z = dot(hb_ref[0], w1)
        q = dot(eb, w2, 1, 1)
        a, da = gelu_both(z)
        s = (da * q).astype(BF)
        gst[g, 1] = dot(a.astype(BF).T, eb).astype(BF)
        gst[g, 0] = dot(ht_s[...], s).astype(BF)
        e_s[...] += dot(s, w1, 1, 1)
        core_copy(i).start()


def shard_map_of(first, count, i):
    return jnp.clip(i - 8 - first, 0, count - 1), 0, 0


def backward_scatter(w_in, w_out, hs, hl, y, inv):
    last = UNITS - 1

    def layer(i):
        return LAYERS - 1 - jnp.minimum(i, last) // PER

    full = pl.BlockSpec((ROWS, DIM), lambda i: (0, 0))
    dma = pltpu.SemaphoreType.DMA
    return pl.pallas_call(
        functools.partial(bwd_kernel, inv),
        grid=(UNITS + DEPTH,),
        in_specs=[
            pl.BlockSpec((1, DIM, TILE), lambda i: (layer(i), 0, jnp.minimum(i, last) % PER)),
            pl.BlockSpec((1, TILE, DIM), lambda i: (layer(i), jnp.minimum(i, last) % PER, 0)),
            pl.BlockSpec((1, ROWS, DIM), lambda i: (layer(i), 0, 0)),
            full, full,
        ],
        out_specs=[pl.BlockSpec(memory_space=pl.ANY)] + [
            pl.BlockSpec((1, 256, 128), functools.partial(shard_map_of, f, n)) for f, n in SPANS[1:]],
        out_shape=[jax.ShapeDtypeStruct((SPANS[0][1], 2, 512, 512), BF)] + [
            jax.ShapeDtypeStruct((n, 256, 128), BF) for _, n in SPANS[1:]],
        scratch_shapes=[
            pltpu.VMEM((ROWS, DIM), F32), pltpu.VMEM((ROWS, DIM), BF), pltpu.VMEM((DIM, ROWS), BF),
            pltpu.VMEM((4, 2, 512, 512), BF), pltpu.VMEM((RING, 512, 512), BF), pltpu.VMEM((ARING, 512, 512), BF),
            pltpu.VMEM((RING, 512, 512), BF),
            pltpu.VMEM((RING, 256, 512), BF), pltpu.VMEM((RING, 256, 256), BF), pltpu.VMEM((RING, 256, 128), BF),
            pltpu.VMEM((RING, 256, 128), BF),
        ] + [dma(n) for n in ((4,), (RING,)) + ((4, 3), (RING, 3)) * 3] * 2 + [dma((4, 2))],
        compiler_params=pltpu.CompilerParams(
            vmem_limit_bytes=VMEM_LIMIT, collective_id=0, has_side_effects=True),
        name="bwd_scatter",
    )(w_in, w_out, hs, hl, y)


def upd_kernel(lo, hi, nalias, h_ref, g_hbm, *rest):
    ins, rest = rest[:4], rest[4 + nalias:]
    outs, ho_ref, (h_s, hb_s, wb1, wb2, sums, gbuf), bufs, (isem, osem) = (
        rest[:4], rest[4], rest[5:11], rest[11:15], rest[15:])
    i = pl.program_id(0)
    n = (hi - lo) * PER

    def window(ref, u, c):
        tile = pl.ds(pl.multiple_of(lax.rem(u, PER) * TILE, TILE), TILE)
        layer = lo + lax.div(u, PER)
        return ref.at[layer, tile, :] if c else ref.at[layer, :, tile]

    def place_of(u):
        return (hi - lo - 1 - lax.div(u, PER)) * PER + lax.rem(u, PER)

    def loads(u):
        slot = lax.rem(u, SLOTS)
        src = g_hbm.at[place_of(u)] if lo == 0 else g_hbm.at[:, place_of(u)]
        return [pltpu.make_async_copy(window(r, u, a % 2), bufs[a].at[slot], isem.at[slot, a])
                for a, r in enumerate(ins)] + [pltpu.make_async_copy(src, gbuf.at[slot], isem.at[slot, 4])]

    def stores(u):
        slot = lax.rem(u, SLOTS)
        return [pltpu.make_async_copy(bufs[a].at[slot], window(r, u, a % 2), osem.at[slot, a])
                for a, r in enumerate(outs)]

    @pl.when(i == 0)
    def _():
        for u in range(AHEAD):
            for c in loads(u):
                c.start()
        h_s[...] = h_ref[...].astype(F32)

    @pl.when(i >= AHEAD)
    def _():
        for c in stores(i - AHEAD):
            c.wait()

    @pl.when(i + AHEAD < n)
    def _():
        for c in loads(i + AHEAD):
            c.start()

    @pl.when(lax.rem(i, PER) == 0)
    def _():
        hb_s[...] = h_s[...].astype(BF)

    slot = lax.rem(i, SLOTS)
    for c in loads(i):
        c.wait()

    if lo:
        rot = lax.rem((LAYERS - hi) * PER + place_of(i), 3)

        @pl.loop(0, 8)
        def _(q):
            for k in range(3):
                bits = []
                for p in range(3):
                    a = lax.rem(rot + k + p, 3)
                    stride = lax.div(a * a + a + 2, 2)
                    bits.append(lax.rem(lax.div(q, stride), 2))
                rows = pl.ds(pl.multiple_of(START[k] + bits[0] * HALF[k], 16), HALF[k])
                cols = pl.ds(pl.multiple_of(bits[1] * 256 + bits[2] * 128, 128), 128)
                for c in range(2):
                    sums[c, rows, cols] = gbuf[slot, 2 * q + c, pl.ds(HSTART[k], HALF[k]), :]

    @pl.loop(0, 16)
    def _(r):
        rows = pl.ds(pl.multiple_of(r * 32, 32), 32)
        for c, wb in enumerate((wb1, wb2)):
            w, m = bufs[c], bufs[2 + c]
            g = sums[c, rows, :] if lo else gbuf[slot, c, rows, :]
            mn = MU * m[slot, rows, :] + g.astype(F32)
            wn = w[slot, rows, :] - STEP * mn
            m[slot, rows, :] = mn
            w[slot, rows, :] = wn
            wb[rows, :] = wn.astype(BF)

    for c in stores(i):
        c.start()
    z = dot(hb_s[...], wb1[...])
    h_s[...] += dot(gelu(z).astype(BF), wb2[...])

    @pl.when(i == n - 1)
    def _():
        ho_ref[...] = h_s[...]
        for u in range(n - AHEAD, n):
            for c in stores(u):
                c.wait()


def update_forward(lo, hi, h, g, weights, prev):
    n = (hi - lo) * PER
    full = pl.BlockSpec((ROWS, DIM), lambda i: (0, 0))
    hbm = pl.BlockSpec(memory_space=pl.ANY)
    nalias = len(prev)
    s1 = jax.ShapeDtypeStruct((LAYERS, DIM, HID), F32)
    s2 = jax.ShapeDtypeStruct((LAYERS, HID, DIM), F32)
    gshape = (2, 512, 512) if lo == 0 else (16, 256, 128)
    tile = (TILE, DIM)
    return pl.pallas_call(
        functools.partial(upd_kernel, lo, hi, nalias),
        grid=(n,),
        in_specs=[full] + [hbm] * (5 + nalias),
        out_specs=[hbm] * 4 + [full],
        out_shape=[s1, s2, s1, s2, jax.ShapeDtypeStruct((ROWS, DIM), F32)],
        input_output_aliases={6 + a: a for a in range(nalias)},
        scratch_shapes=[
            pltpu.VMEM((ROWS, DIM), F32), pltpu.VMEM((ROWS, DIM), BF), pltpu.VMEM(tile, BF), pltpu.VMEM(tile, BF),
            pltpu.VMEM((2,) + tile, BF), pltpu.VMEM((SLOTS,) + gshape, BF),
        ] + [pltpu.VMEM((SLOTS,) + tile, F32)] * 4 + [
            pltpu.SemaphoreType.DMA((SLOTS, 5)), pltpu.SemaphoreType.DMA((SLOTS, 4))],
        compiler_params=pltpu.CompilerParams(vmem_limit_bytes=VMEM_LIMIT),
        cost_estimate=pl.CostEstimate(flops=n * 4 * 512**3, bytes_accessed=n * 9 * 2**20, transcendentals=0),
        name="upd_fwd",
    )(h, g, *weights, *prev)


def solution(mesh):
    groups = mesh.shape["data"]
    rows_spec = P("data", None)

    def local_steps(w_in, w_out, mom_in, mom_out, x_first, y_first, x_second, y_second):
        hs, hl = forward_first(x_first, w_in, w_out)
        first, *shards = backward_scatter(w_in, w_out, hs, hl, y_first, 1.0 / (ROWS * groups * DIM))
        gathered = [first] + [lax.all_gather(part, "data", axis=0, tiled=False) for part in shards]
        h, prev = x_second, ()
        for (lo, hi), g in zip(CHUNKS, gathered):
            *prev, h = update_forward(lo, hi, h, g, (w_in, w_out, mom_in, mom_out), tuple(prev))
        row_diff = h - y_second.astype(F32)
        loss_rows = jnp.sum(row_diff * row_diff, axis=-1) / (2 * DIM)
        return prev[0], prev[1], prev[2], prev[3], loss_rows, h

    return jax.shard_map(
        local_steps, mesh=mesh,
        in_specs=(P(), P(), P(), P(), rows_spec, rows_spec, rows_spec, rows_spec),
        out_specs=(P(), P(), P(), P(), P("data"), rows_spec), check_vma=False)
```
